32 devices in a mesh: grp: 8 (over z, core), tp: 4 (over y, x).
Axes of the slice: x: 2, y: 2, z: 4, core: 2. Of those that a mesh axis runs over, the one named last changes fastest.
Arguments:
- tokens: bfloat16 [8192, 8192], P('grp'), may hold values from -12 to 12
- joined_weight: bfloat16 [8192, 10240], P(('grp', 'tp')), may hold values from -1.14904852 to 1.14904852
- rollout_lengths: int32 [64], P('grp'), may hold values from 1 to 128
- prompt_of: int32 [64, 1], P('grp'), may hold values from 0 to 7
- score_weight: bfloat16 [8192], P('tp'), may hold values from -0.52734375 to 0.52734375
Outputs:
- attention: bfloat16 [8192, 8192], P('grp', 'tp')
- advantages: float32 [64], P('grp')
The draws below stay inside these ranges and needn't reach their ends.
All inputs are finite; a program needn't handle non-finite values.
Results may differ from the reference program's by a relative error of at most 0.012.
The reference program's roundings to bfloat16 on the way count: a program that leaves them out, or rounds other values in their place, can miss the bound.
Values may be sent and summed in bfloat16 or wider, within the bound.
A program may use at most 128 MiB of HBM per device.

```python
import jax
import jax.numpy as jnp
from jax import lax

MODEL_WIDTH = 8192
QUERY_HEADS = 64
KV_HEAD_COUNT = 8
HEAD_SIZE = 128
ROLL = 8
SLOT = 128
TOK_G = 1024
TOKENS = 8192
ROLLOUTS = 64
PROMPTS = 8
COLS = 10240
N_GRP = 8


def draw_tokens(key, part):
    values = jnp.clip(jax.random.normal(key, (TOKENS, MODEL_WIDTH), jnp.float32), -6.0, 6.0)
    return values.astype(jnp.bfloat16)


def draw_joined_weight(key, part):
    head_ratio = QUERY_HEADS // KV_HEAD_COUNT
    base_offset = jnp.clip(jax.random.normal(key, (MODEL_WIDTH, KV_HEAD_COUNT, head_ratio + 2, HEAD_SIZE), jnp.float32), -6.0, 6.0) * MODEL_WIDTH ** (-0.5)
    return base_offset.reshape(MODEL_WIDTH, COLS).astype(jnp.bfloat16)


def set_ends(entries, own_key, least, top_value):
    longest = entries.shape.index(max(entries.shape))
    spots = []
    for shift in (0, 1):
        where = [jax.random.randint(jax.random.fold_in(own_key, axis), (), 0, length) for axis, length in enumerate(entries.shape)]
        where[longest] = (where[longest] + shift) % entries.shape[longest]
        spots.append(tuple(where))
    return entries.at[spots[0]].set(least).at[spots[1]].set(top_value)


def levels(stream_key, extent, shards, low, high):
    level = 1.0
    for dim, parts in shards:
        steps = jax.random.uniform(jax.random.fold_in(jax.random.fold_in(stream_key, 6), dim), (parts,), jnp.float32, low / len(shards), high / len(shards))
        level = level * jnp.repeat(jnp.exp(steps), extent[dim] // parts).reshape((-1,) + (1,) * (len(extent) - 1 - dim))
    return level


def different_ones(rng, rows, amount, top, lift):
    sequence = jax.random.permutation(jax.random.fold_in(rng, 1), amount)
    boost = sequence
    for power in range(3):
        boost = boost * boost // amount
    boost = boost * lift // amount
    lots = jax.random.randint(jax.random.fold_in(rng, 2), (rows, amount), 0, 4096) + boost
    fixed_rows = jax.random.permutation(jax.random.fold_in(rng, 3), rows)[jnp.arange(amount) % rows]
    lots = jnp.where(jnp.arange(rows)[:, None] == fixed_rows[None, :], 1 << 14, lots)
    priority = lots * amount + jnp.arange(amount)
    return lax.top_k(priority.astype(jnp.int32), top)[1].astype(jnp.int32)


def normal_values(key, dims, deviation, limit, pieces=(), kind=jnp.bfloat16):
    factor_of = levels(key, dims, pieces, -0.22, 0.18) if pieces else 1.0
    result = jax.random.normal(key, dims, jnp.float32) * deviation * factor_of
    return jnp.minimum(jnp.maximum(result, -limit), limit).astype(kind)


def setup_inputs(seed: int = 0) -> dict:
    key_of = jax.random.split(jax.random.key(seed), 6)
    return {
        "tokens": draw_tokens(jax.random.fold_in(key_of[5], 71), 0),
        "joined_weight": draw_joined_weight(jax.random.fold_in(key_of[5], 71), 0),
        "rollout_lengths": set_ends(jax.random.randint(key_of[2], (ROLLOUTS,), 1, SLOT + 1), jax.random.fold_in(key_of[2], 1), 1, SLOT).astype(jnp.int32),
        "prompt_of": different_ones(key_of[3], ROLLOUTS, PROMPTS, 1, 0),
        "score_weight": normal_values(key_of[4], (QUERY_HEADS * HEAD_SIZE,), (8.0 / (QUERY_HEADS * HEAD_SIZE) ** 0.5), 0.52734375, ((0, 4),)),
    }


def attend(joined_matrix, rollout_length_list):
    head_ratio = QUERY_HEADS // KV_HEAD_COUNT
    slot_index = joined_matrix.shape[0] // rollout_length_list.shape[0]
    reshaped_tensor = joined_matrix.reshape(rollout_length_list.shape[0], slot_index, KV_HEAD_COUNT, head_ratio + 2, HEAD_SIZE).astype(jnp.float32)
    queries = reshaped_tensor[:, :, :, :head_ratio, :]
    key_heads = reshaped_tensor[:, :, :, head_ratio, :]
    value_heads = reshaped_tensor[:, :, :, head_ratio + 1, :]
    scores = jnp.einsum('rsgah,rtgh->rgast', queries, key_heads) * HEAD_SIZE ** (-0.5)
    positions = jnp.arange(slot_index)
    allowed = (positions[None, None, :] <= positions[None, :, None]) & (positions[None, None, :] < rollout_length_list[:, None, None])
    scores = jnp.where(allowed[:, None, None], scores, jnp.float32(-1e+30))
    peak = lax.optimization_barrier(jnp.max(scores, axis=-1, keepdims=True))
    expo = jnp.exp(scores - peak)
    probs = (expo / lax.optimization_barrier(jnp.sum(expo, axis=-1, keepdims=True))).astype(jnp.bfloat16)
    mixed = jnp.einsum('rgast,rtgh->rsgah', probs.astype(jnp.float32), value_heads)
    return mixed.reshape(joined_matrix.shape[0], QUERY_HEADS * HEAD_SIZE).astype(jnp.bfloat16)

def reference(tokens, joined_weight, rollout_lengths, prompt_of, score_weight):

    def one_group(items):
        group_tokens, rollout_length_list = items
        joined_matrix = jnp.dot(group_tokens, joined_weight, preferred_element_type=jnp.float32).astype(jnp.bfloat16)
        attention = attend(joined_matrix, rollout_length_list)
        token_score = jnp.dot(attention, score_weight, preferred_element_type=jnp.float32)
        valid = jnp.arange(SLOT)[None, :] < rollout_length_list[:, None]
        reward = lax.optimization_barrier(jnp.sum(jnp.where(valid, token_score.reshape(ROLL, SLOT), jnp.float32(0.0)), axis=1)) / rollout_length_list.astype(jnp.float32)
        return (attention, reward)
    attention, rewards = lax.map(one_group, (tokens.reshape(N_GRP, TOK_G, MODEL_WIDTH), rollout_lengths.reshape(N_GRP, ROLL)))
    attention = attention.reshape(TOKENS, QUERY_HEADS * HEAD_SIZE)
    rewards = rewards.reshape(ROLLOUTS)
    onehot = (prompt_of == jnp.arange(PROMPTS)[None, :]).astype(jnp.float32)
    counts = lax.optimization_barrier(jnp.sum(onehot, axis=0))
    totals = lax.optimization_barrier(jnp.sum(onehot * rewards[:, None], axis=0))
    squares = lax.optimization_barrier(jnp.sum(onehot * (rewards * rewards)[:, None], axis=0))
    divisor = jnp.maximum(counts, 1.0)
    average = totals / divisor
    spread = squares / divisor - average * average
    own_mean = lax.optimization_barrier(jnp.sum(onehot * average[None, :], axis=1))
    own_var = lax.optimization_barrier(jnp.sum(onehot * spread[None, :], axis=1))
    advantages = (rewards - own_mean) / jnp.sqrt(own_var + 0.25)
    return (attention, advantages)
```

```python
import functools

import jax
import jax.numpy as jnp
from jax import lax
from jax.experimental import pallas as pl
from jax.experimental.pallas import tpu as pltpu
from jax.sharding import PartitionSpec as P

QUERY_HEADS = 64
KV_HEAD_COUNT = 8
HEAD_SIZE = 128
CORES = 2
CHUNKS = 5


def attend_kernel(groups, chunks, lengths_ref, weight_ref, *refs):
    own = refs[:chunks]
    extra = refs[chunks : 2 * chunks]
    out_ref, reward_ref = refs[2 * chunks :]
    ratio = QUERY_HEADS // KV_HEAD_COUNT
    per_chunk = own[0].shape[1] // HEAD_SIZE
    slot = own[0].shape[0]
    length = lengths_ref[pl.program_id(0)]

    def head(index):
        c, h = divmod(index, per_chunk)
        cols = slice(h * HEAD_SIZE, (h + 1) * HEAD_SIZE)
        return (own[c][:, cols] + extra[c][:, cols].astype(jnp.float32)).astype(jnp.bfloat16)

    s_pos = lax.broadcasted_iota(jnp.int32, (slot, slot), 0)
    t_pos = lax.broadcasted_iota(jnp.int32, (slot, slot), 1)
    allowed = (t_pos <= s_pos) & (t_pos < length)
    live = lax.broadcasted_iota(jnp.int32, (slot, HEAD_SIZE), 0) < length
    total = jnp.zeros((slot, HEAD_SIZE), jnp.float32)
    for g in range(groups):
        base = g * (ratio + 2)
        key = head(base + ratio)
        value = head(base + ratio + 1)
        for a in range(ratio):
            scores = lax.dot_general(
                head(base + a), key, (((1,), (1,)), ((), ())), preferred_element_type=jnp.float32
            ) * HEAD_SIZE ** (-0.5)
            scores = jnp.where(allowed, scores, jnp.float32(-1e30))
            peak = jnp.max(scores, axis=-1, keepdims=True)
            expo = jnp.exp(scores - peak)
            probs = (expo / jnp.sum(expo, axis=-1, keepdims=True)).astype(jnp.bfloat16)
            mixed = jnp.dot(probs, value, preferred_element_type=jnp.float32).astype(jnp.bfloat16)
            cols = slice((g * ratio + a) * HEAD_SIZE, (g * ratio + a + 1) * HEAD_SIZE)
            out_ref[:, cols] = mixed
            total += mixed.astype(jnp.float32) * weight_ref[:, cols].astype(jnp.float32)
    summed = jnp.sum(jnp.where(live, total, jnp.float32(0.0)), axis=0, keepdims=True)
    summed = jnp.sum(summed, axis=1, keepdims=True)
    reward_ref[...] = jnp.broadcast_to(summed[None], reward_ref.shape)


def attend(own, extra, lengths, score_weight):
    rows, width = own[0].shape
    rollouts = lengths.shape[0]
    slot = rows // rollouts
    chunks = len(own)
    features = score_weight.shape[0]
    ratio = QUERY_HEADS // KV_HEAD_COUNT
    block = pl.BlockSpec((slot, width), lambda r, *_: (r, 0))
    attention, reward = pl.pallas_call(
        functools.partial(attend_kernel, features // (ratio * HEAD_SIZE), chunks),
        grid_spec=pltpu.PrefetchScalarGridSpec(
            num_scalar_prefetch=1,
            grid=(rollouts,),
            in_specs=[pl.BlockSpec((1, features), lambda r, *_: (0, 0))] + [block] * (2 * chunks),
            out_specs=[
                pl.BlockSpec((slot, features), lambda r, *_: (r, 0)),
                pl.BlockSpec((1, 8, HEAD_SIZE), lambda r, *_: (r, 0, 0)),
            ],
        ),
        out_shape=[
            jax.ShapeDtypeStruct((rows, features), jnp.bfloat16),
            jax.ShapeDtypeStruct((rollouts, 8, HEAD_SIZE), jnp.float32),
        ],
        cost_estimate=pl.CostEstimate(
            flops=4 * rows * slot * features, bytes_accessed=8 * rows * features, transcendentals=0
        ),
    )(lengths, score_weight.reshape(1, features), *own, *extra)
    return attention, reward[:, 0, 0]


def after_all(values, *earlier):
    return lax.optimization_barrier((tuple(values), earlier))[0]


def after(value, *earlier):
    return after_all((value,), *earlier)[0]


def shards(tokens, joined_weight, rollout_lengths, prompt_of, score_weight):
    grp_count = lax.axis_size("grp")
    tp_count = lax.axis_size("tp")
    n = grp_count // CORES
    g = lax.axis_index("grp")
    t = lax.axis_index("tp")
    z, core = g // CORES, g % CORES
    rows, depth = tokens.shape
    own_rows = joined_weight.shape[0]
    half_rows = own_rows * tp_count
    plane_rows = half_rows * CORES
    columns = joined_weight.shape[1] // tp_count
    width = columns // CHUNKS

    def along(x, pairs):
        return lax.ppermute(
            x, "grp", [(CORES * a + c, CORES * b + c) for a, b in pairs for c in range(CORES)]
        )

    def swap(x):
        return lax.ppermute(x, "grp", [(i, i ^ 1) for i in range(grp_count)])

    def exchange(x, d):
        return lax.ppermute(x, "tp", [(i, i ^ d) for i in range(tp_count)])

    prompts = lax.all_gather(prompt_of, "grp", axis=0, tiled=True)

    far = plane_rows * (n - 2)
    far_start = jnp.where(z < n // 2, 2 * plane_rows, 0)
    part = rows // tp_count
    token_part = lax.dynamic_slice(tokens, (t * part, far_start), (part, far))
    token_part = along(token_part, [(0, 1), (n - 1, n - 2)])
    far_tokens = lax.all_gather(token_part, "tp", axis=0, tiled=True)

    locals_, ones, twos, own_out, products = [], [], [], [], []
    extra_out = []
    for q in range(CHUNKS):
        weight = joined_weight
        if q:
            weight = after(weight, locals_[q - 1])
        local = jnp.zeros((half_rows, width), jnp.bfloat16)
        for d in range(tp_count):
            piece = lax.dynamic_slice(weight, (0, (t ^ d) * columns + q * width), (own_rows, width))
            if d:
                piece = exchange(piece, d)
            local = lax.dynamic_update_slice(local, piece, ((t ^ d) * own_rows, 0))
        locals_.append(local)
        if q >= 2:
            local = after(local, *ones[q - 2])
        if q >= 3:
            local = after(local, *twos[q - 3])
        left, right = {0: local}, {0: local}
        for s in range(1, n - 1):
            first = 0 if s == 1 else 1
            pairs = [(r + 1, r) for r in range(first, n - s)]
            source = [left[s - 1], right[s - 1]]
            if s == 2:
                if q >= 2:
                    source = after_all(source, own_out[q - 2])
                if q >= 3:
                    source = after_all(source, products[q - 3])
            left[s] = along(source[0], pairs)
            right[s] = along(source[1], [(n - 1 - a, n - 1 - b) for a, b in pairs])
        ones.append((left[1], right[1]))
        twos.append((left[n - 2], right[n - 2]))
        whole = jnp.zeros((depth, width), jnp.bfloat16)
        for k in range(n):
            if k == 0:
                block = local
            else:
                both = [m[i] for m, i in ((left, k), (right, n - k)) if i in m]
                block = both[0] + both[1] if len(both) == 2 else both[0]
            base = (z + k) % n * plane_rows
            whole = lax.dynamic_update_slice(whole, block, (base + core * half_rows, 0))
            whole = lax.dynamic_update_slice(whole, swap(block), (base + (1 - core) * half_rows, 0))
        beyond = lax.dynamic_slice(whole, (far_start, 0), (far, width))
        product = jnp.dot(far_tokens, beyond, preferred_element_type=jnp.float32)
        product = product.astype(jnp.bfloat16)
        products.append(product)
        extra_out.append(along(product, [(1, 0), (n - 2, n - 1)]))
        if q == CHUNKS - 1:
            whole = after(whole, product)
        own_out.append(jnp.dot(tokens, whole, preferred_element_type=jnp.float32))

    attention, reward = attend(own_out, extra_out, rollout_lengths, score_weight)
    reward = reward / rollout_lengths.astype(jnp.float32)
    gathered = lax.all_gather(reward, ("grp", "tp"), axis=0)
    everyone = jnp.sum(gathered.reshape(grp_count, tp_count, -1), axis=1).reshape(-1)
    labels = jnp.arange(grp_count)[None, :]
    onehot = (prompts == labels).astype(jnp.float32)
    counts = jnp.sum(onehot, axis=0)
    totals = jnp.sum(onehot * everyone[:, None], axis=0)
    squares = jnp.sum(onehot * (everyone * everyone)[:, None], axis=0)
    divisor = jnp.maximum(counts, 1.0)
    average = totals / divisor
    spread = squares / divisor - average * average
    mine = (prompt_of == labels).astype(jnp.float32)
    own_mean = jnp.sum(mine * average[None, :], axis=1)
    own_var = jnp.sum(mine * spread[None, :], axis=1)
    rewards = lax.dynamic_slice(everyone, (g * reward.shape[0],), reward.shape)
    advantages = (rewards - own_mean) / jnp.sqrt(own_var + 0.25)
    return (attention, advantages)


def solution(mesh):
    return jax.shard_map(
        shards,
        mesh=mesh,
        in_specs=(P("grp", None), P(("grp", "tp"), None), P("grp"), P("grp", None), P("tp")),
        out_specs=(P("grp", "tp"), P("grp")),
        check_vma=False,
    )
```

```python
import functools

import jax
import jax.numpy as jnp
from jax import lax
from jax.experimental import pallas as pl
from jax.experimental.pallas import tpu as pltpu
from jax.sharding import PartitionSpec as P

QUERY_HEADS = 64
KV_HEAD_COUNT = 8
HEAD_SIZE = 128
CORES = 2
CHUNKS = 5


def attend_kernel(groups, chunks, lengths_ref, flag_ref, weight_ref, own, extra, out_ref, reward_ref):
    ratio = QUERY_HEADS // KV_HEAD_COUNT
    per_chunk = own.shape[2] // HEAD_SIZE
    slot = own.shape[1]
    length = lengths_ref[pl.program_id(0)]
    at_end = flag_ref[0] > 0

    def head(index):
        c, h = divmod(index, per_chunk)
        cols = slice(h * HEAD_SIZE, (h + 1) * HEAD_SIZE)
        added = jnp.where(at_end, extra[c, :, cols].astype(jnp.float32), jnp.float32(0.0))
        return (own[c, :, cols] + added).astype(jnp.bfloat16)

    s_pos = lax.broadcasted_iota(jnp.int32, (slot, slot), 0)
    t_pos = lax.broadcasted_iota(jnp.int32, (slot, slot), 1)
    allowed = ((t_pos <= s_pos) & (t_pos < length))[None]
    live = lax.broadcasted_iota(jnp.int32, (slot, HEAD_SIZE), 0) < length
    total = jnp.zeros((slot, HEAD_SIZE), jnp.float32)
    for g in range(groups):
        base = g * (ratio + 2)
        key = head(base + ratio)
        value = head(base + ratio + 1)
        queries = jnp.concatenate([head(base + a) for a in range(ratio)], axis=0)
        scores = lax.dot_general(
            queries, key, (((1,), (1,)), ((), ())), preferred_element_type=jnp.float32
        ) * HEAD_SIZE ** (-0.5)
        scores = jnp.where(allowed, scores.reshape(ratio, slot, slot), jnp.float32(-1e30))
        expo = jnp.exp(scores - jnp.max(scores, axis=-1, keepdims=True))
        probs = expo * (1.0 / jnp.sum(expo, axis=-1, keepdims=True))
        probs = probs.astype(jnp.bfloat16).reshape(ratio * slot, slot)
        mixed = jnp.dot(probs, value, preferred_element_type=jnp.float32).astype(jnp.bfloat16)
        for a in range(ratio):
            part = mixed[a * slot : (a + 1) * slot]
            cols = slice((g * ratio + a) * HEAD_SIZE, (g * ratio + a + 1) * HEAD_SIZE)
            out_ref[:, cols] = part
            total += part.astype(jnp.float32) * weight_ref[:, cols].astype(jnp.float32)
    summed = jnp.sum(jnp.where(live, total, jnp.float32(0.0)), axis=0, keepdims=True)
    summed = jnp.sum(summed, axis=1, keepdims=True)
    reward_ref[...] = jnp.broadcast_to(summed[None], reward_ref.shape)


def attend(own, extra, lengths, flag, score_weight):
    chunks, rows, width = own.shape
    rollouts = lengths.shape[0]
    slot = rows // rollouts
    features = score_weight.shape[0]
    ratio = QUERY_HEADS // KV_HEAD_COUNT
    block = pl.BlockSpec((chunks, slot, width), lambda r, *_: (0, r, 0))
    attention, reward = pl.pallas_call(
        functools.partial(attend_kernel, features // (ratio * HEAD_SIZE), chunks),
        grid_spec=pltpu.PrefetchScalarGridSpec(
            num_scalar_prefetch=2,
            grid=(rollouts,),
            in_specs=[pl.BlockSpec((1, features), lambda r, *_: (0, 0)), block, block],
            out_specs=[
                pl.BlockSpec((slot, features), lambda r, *_: (r, 0)),
                pl.BlockSpec((1, 8, HEAD_SIZE), lambda r, *_: (r, 0, 0)),
            ],
        ),
        out_shape=[
            jax.ShapeDtypeStruct((rows, features), jnp.bfloat16),
            jax.ShapeDtypeStruct((rollouts, 8, HEAD_SIZE), jnp.float32),
        ],
    )(lengths, flag, score_weight.reshape(1, features), own, extra)
    return attention, reward[:, 0, 0]


def project_kernel(
    n, tp_count, tokens, weight, own_out, extra, gath, far, prod,
    tok_v, far_v, w_v, acc, pbuf, send, recv, loads, w_sem, misc,
):
    g = lax.axis_index("grp")
    t = lax.axis_index("tp")
    z, core = g // CORES, g % CORES
    rows, depth = tokens.shape
    chunks, _, width = gath.shape
    own_rows = weight.shape[0]
    half = own_rows * tp_count
    plane = half * CORES
    columns = width * chunks
    part = rows // tp_count
    far_cols = far.shape[1]
    steps = n - 2
    inner = (z >= 1) & (z <= n - 2)
    helper = (z == 1) | (z == n - 2)
    at_end = (z == 0) | (z == n - 1)
    first_far = jnp.where(z < n // 2, 2, 0)
    ids = {}

    def sem(key):
        return ids.setdefault(key, len(ids))

    def remote(key, src, dst, device):
        i = sem(key)
        return pltpu.make_async_remote_copy(
            src_ref=src, dst_ref=dst, send_sem=send.at[i], recv_sem=recv.at[i],
            device_id=device, device_id_type=pl.DeviceIdType.MESH,
        )

    sends = []

    def start(cond, key, src, dst, device):
        @pl.when(cond)
        def _():
            remote(key, src, dst, device).start()

        sends.append((cond, key, src, dst, device))

    def arrived(cond, key, dst):
        @pl.when(cond)
        def _():
            remote(key, dst, dst, (g, t)).wait_recv()

    always = z >= 0
    sibling = (g + 1 - 2 * core, t)

    def piece(q, who):
        return gath.at[q, pl.ds(pl.multiple_of(z * plane + core * half + who * own_rows, own_rows), own_rows)]

    def block(q, p, c):
        return gath.at[q, pl.ds(pl.multiple_of(p * plane + c * half, half), half)]

    def columns_of(who, q):
        return weight.at[:, pl.ds(pl.multiple_of(who * columns + q * width, width), width)]

    def scatter(q):
        pltpu.make_async_copy(columns_of(t, q), piece(q, t), loads.at[q]).start()
        for d in range(1, tp_count):
            start(always, ("a", q, d), columns_of(t ^ d, q), piece(q, t), (g, t ^ d))

    def gathered(q):
        pltpu.make_async_copy(columns_of(t, q), piece(q, t), loads.at[q]).wait()
        for d in range(1, tp_count):
            arrived(always, ("a", q, d), piece(q, t ^ d))

    def launch(q):
        mine = block(q, z, core)
        start(z >= 1, ("l", q, 1), mine, mine, (g - CORES, t))
        start(z <= n - 2, ("r", q, 1), mine, mine, (g + CORES, t))
        start(always, ("s", q), mine, mine, sibling)

    def has(side, s):
        reach = (z + s <= n - 1) if side == "l" else (z - s >= 0)
        return reach if s == 1 else reach & inner

    def forward(q, s):
        for side, sign in (("l", 1), ("r", -1)):
            here = jnp.clip(z + sign * s, 0, n - 1)
            got = block(q, here, core)
            arrived(has(side, s), (side, q, s), got)
            if s < steps:
                more = (z >= 2) if side == "l" else (z <= n - 3)
                start(has(side, s) & more, (side, q, s + 1), got, got, (g - sign * CORES, t))
            start(has(side, s), ("s" + side, q, s), got, got, sibling)

    def swapped(q):
        arrived(always, ("s", q), block(q, z, 1 - core))
        for s in range(1, steps + 1):
            for side, sign in (("l", 1), ("r", -1)):
                here = jnp.clip(z + sign * s, 0, n - 1)
                arrived(has(side, s), ("s" + side, q, s), block(q, here, 1 - core))

    tile = 256

    def gemm(q, lhs, low, high, origin):
        def load(p):
            return pltpu.make_async_copy(
                gath.at[q, pl.ds(pl.multiple_of(p * plane, plane), plane)], w_v.at[p % 2], w_sem.at[p % 2]
            )

        load(low).start()
        acc[...] = jnp.zeros_like(acc)

        def step(p, carry):
            @pl.when(p + 1 < high)
            def _():
                load(p + 1).start()

            load(p).wait()
            cols = pl.ds(pl.multiple_of((p - origin) * plane, plane), plane)

            def rows_step(m, carry):
                at = pl.ds(pl.multiple_of(m * tile, tile), tile)
                acc[at, :] += jnp.dot(lhs[at, cols], w_v[p % 2], preferred_element_type=jnp.float32)
                return carry

            return lax.fori_loop(0, rows // tile, rows_step, carry)

        lax.fori_loop(low, high, step, 0)

    def compute(q):
        low = jnp.where(z == n - 1, n - 2, 0)
        high = jnp.where(z == 0, 2, n)
        gemm(q, tok_v, low, high, 0)
        out = pltpu.make_async_copy(acc, own_out.at[q], misc.at[1])
        out.start()
        out.wait()

    def assist(q):
        @pl.when(helper)
        def _():
            gemm(q, far_v, first_far, first_far + steps, first_far)
            pbuf[...] = acc[...].astype(pbuf.dtype)
            out = pltpu.make_async_copy(pbuf, prod.at[q], misc.at[2])
            out.start()
            out.wait()

        start(helper, ("p", q), prod.at[q], extra.at[q], (jnp.where(z == 1, g - CORES, g + CORES), t))

    def token_rows(who):
        return far.at[pl.ds(pl.multiple_of(who * part, part), part)]

    load_tokens = pltpu.make_async_copy(tokens, tok_v, misc.at[0])
    scatter(0)
    scatter(1)
    load_tokens.start()
    gathered(0)
    launch(0)
    far_source = tokens.at[
        pl.ds(pl.multiple_of(t * part, part), part),
        pl.ds(pl.multiple_of(first_far * plane, plane), far_cols),
    ]
    start(at_end, ("t",), far_source, token_rows(t), (jnp.where(z == 0, g + CORES, g - CORES), t))
    gathered(1)
    launch(1)
    load_tokens.wait()
    late = chunks - 2
    for q in range(chunks):
        if q + 2 < chunks:
            scatter(q + 2)
        if q == 1:
            arrived(helper, ("t",), token_rows(t))
            for d in range(1, tp_count):
                start(helper, ("g", d), token_rows(t), token_rows(t), (g, t ^ d))
        forward(q, 1)
        if q + 2 < chunks:
            gathered(q + 2)
            launch(q + 2)
        if q >= 1:
            for s in range(2, steps + 1):
                forward(q - 1, s)
            swapped(q - 1)
            compute(q - 1)
        if q == late:
            for d in range(1, tp_count):
                arrived(helper, ("g", d), token_rows(t ^ d))

            @pl.when(helper)
            def _():
                fill = pltpu.make_async_copy(far, far_v, misc.at[0])
                fill.start()
                fill.wait()

            for early in range(q - 1):
                assist(early)
        if q >= late and q >= 1:
            assist(q - 1)
    last = chunks - 1
    for s in range(2, steps + 1):
        forward(last, s)
    swapped(last)
    assist(last)
    compute(last)
    for q in range(chunks):
        arrived(at_end, ("p", q), extra.at[q])
    for cond, key, src, dst, device in sends:
        @pl.when(cond)
        def _():
            remote(key, src, dst, device).wait_send()


def project(tokens, weight, n, tp_count):
    rows, depth = tokens.shape
    own_rows = weight.shape[0]
    width = weight.shape[1] // tp_count // CHUNKS
    plane = own_rows * tp_count * CORES
    far = plane * (n - 2)
    flows = CHUNKS * (tp_count + 1 + 4 * (n - 2)) + tp_count
    anywhere = pl.BlockSpec(memory_space=pl.ANY)
    own, extra, *_ = pl.pallas_call(
        functools.partial(project_kernel, n, tp_count),
        in_specs=[anywhere] * 2,
        out_specs=[anywhere] * 5,
        out_shape=[
            jax.ShapeDtypeStruct((CHUNKS, rows, width), jnp.float32),
            jax.ShapeDtypeStruct((CHUNKS, rows, width), jnp.bfloat16),
            jax.ShapeDtypeStruct((CHUNKS, depth, width), jnp.bfloat16),
            jax.ShapeDtypeStruct((rows, far), jnp.bfloat16),
            jax.ShapeDtypeStruct((CHUNKS, rows, width), jnp.bfloat16),
        ],
        scratch_shapes=[
            pltpu.VMEM((rows, depth), jnp.bfloat16),
            pltpu.VMEM((rows, far), jnp.bfloat16),
            pltpu.VMEM((2, plane, width), jnp.bfloat16),
            pltpu.VMEM((rows, width), jnp.float32),
            pltpu.VMEM((rows, width), jnp.bfloat16),
            pltpu.SemaphoreType.DMA((flows,)),
            pltpu.SemaphoreType.DMA((flows,)),
            pltpu.SemaphoreType.DMA((CHUNKS,)),
            pltpu.SemaphoreType.DMA((2,)),
            pltpu.SemaphoreType.DMA((3,)),
        ],
        compiler_params=pltpu.CompilerParams(has_side_effects=True, vmem_limit_bytes=60 * 1024 * 1024),
    )(tokens, weight)
    return own, extra


def shards(tokens, joined_weight, rollout_lengths, prompt_of, score_weight):
    grp_count = lax.axis_size("grp")
    tp_count = lax.axis_size("tp")
    n = grp_count // CORES
    g = lax.axis_index("grp")
    z = g // CORES
    own, extra = project(tokens, joined_weight, n, tp_count)
    flag = ((z == 0) | (z == n - 1)).astype(jnp.int32).reshape(1)
    attention, reward = attend(own, extra, rollout_lengths, flag, score_weight)
    reward = reward / rollout_lengths.astype(jnp.float32)
    sent = jnp.stack([reward, prompt_of[:, 0].astype(jnp.float32)])
    gathered = lax.all_gather(sent, ("grp", "tp"), axis=0)
    gathered = gathered.reshape(grp_count, tp_count, 2, -1)
    everyone = jnp.sum(gathered[:, :, 0], axis=1).reshape(-1)
    prompts = gathered[:, 0, 1].reshape(-1, 1).astype(jnp.int32)
    labels = jnp.arange(grp_count)[None, :]
    onehot = (prompts == labels).astype(jnp.float32)
    counts = jnp.sum(onehot, axis=0)
    totals = jnp.sum(onehot * everyone[:, None], axis=0)
    squares = jnp.sum(onehot * (everyone * everyone)[:, None], axis=0)
    divisor = jnp.maximum(counts, 1.0)
    average = totals / divisor
    spread = squares / divisor - average * average
    mine = (prompt_of == labels).astype(jnp.float32)
    own_mean = jnp.sum(mine * average[None, :], axis=1)
    own_var = jnp.sum(mine * spread[None, :], axis=1)
    rewards = lax.dynamic_slice(everyone, (g * reward.shape[0],), reward.shape)
    advantages = (rewards - own_mean) / jnp.sqrt(own_var + 0.25)
    return (attention, advantages)


def solution(mesh):
    return jax.shard_map(
        shards,
        mesh=mesh,
        in_specs=(P("grp", None), P(("grp", "tp"), None), P("grp"), P("grp", None), P("tp")),
        out_specs=(P("grp", "tp"), P("grp")),
        check_vma=False,
    )
```

```python
import functools

import jax
import jax.numpy as jnp
from jax import lax
from jax.experimental import pallas as pl
from jax.experimental.pallas import tpu as pltpu
from jax.sharding import PartitionSpec as P

QUERY_HEADS = 64
KV_HEAD_COUNT = 8
HEAD_SIZE = 128
CORES = 2
CHUNKS = 5


def attend_kernel(groups, chunks, lengths_ref, flag_ref, weight_ref, own, extra, out_ref, reward_ref):
    ratio = QUERY_HEADS // KV_HEAD_COUNT
    per_chunk = own.shape[2] // HEAD_SIZE
    slot = own.shape[1]
    length = lengths_ref[pl.program_id(0)]
    at_end = flag_ref[0] > 0

    def head(index):
        c, h = divmod(index, per_chunk)
        cols = slice(h * HEAD_SIZE, (h + 1) * HEAD_SIZE)
        added = jnp.where(at_end, extra[c, :, cols].astype(jnp.float32), jnp.float32(0.0))
        return (own[c, :, cols] + added).astype(jnp.bfloat16)

    s_pos = lax.broadcasted_iota(jnp.int32, (slot, slot), 0)
    t_pos = lax.broadcasted_iota(jnp.int32, (slot, slot), 1)
    allowed = ((t_pos <= s_pos) & (t_pos < length))[None]
    live = lax.broadcasted_iota(jnp.int32, (slot, HEAD_SIZE), 0) < length
    total = jnp.zeros((slot, HEAD_SIZE), jnp.float32)
    for g in range(groups):
        base = g * (ratio + 2)
        key = head(base + ratio)
        value = head(base + ratio + 1)
        queries = jnp.concatenate([head(base + a) for a in range(ratio)], axis=0)
        scores = lax.dot_general(
            queries, key, (((1,), (1,)), ((), ())), preferred_element_type=jnp.float32
        ) * HEAD_SIZE ** (-0.5)
        scores = jnp.where(allowed, scores.reshape(ratio, slot, slot), jnp.float32(-1e30))
        expo = jnp.exp(scores - jnp.max(scores, axis=-1, keepdims=True))
        probs = expo * (1.0 / jnp.sum(expo, axis=-1, keepdims=True))
        probs = probs.astype(jnp.bfloat16).reshape(ratio * slot, slot)
        mixed = jnp.dot(probs, value, preferred_element_type=jnp.float32).astype(jnp.bfloat16)
        for a in range(ratio):
            part = mixed[a * slot : (a + 1) * slot]
            cols = slice((g * ratio + a) * HEAD_SIZE, (g * ratio + a + 1) * HEAD_SIZE)
            out_ref[:, cols] = part
            total += part.astype(jnp.float32) * weight_ref[:, cols].astype(jnp.float32)
    summed = jnp.sum(jnp.where(live, total, jnp.float32(0.0)), axis=0, keepdims=True)
    summed = jnp.sum(summed, axis=1, keepdims=True)
    reward_ref[...] = jnp.broadcast_to(summed[None], reward_ref.shape)


def attend(own, extra, lengths, flag, score_weight):
    chunks, rows, width = own.shape
    rollouts = lengths.shape[0]
    slot = rows // rollouts
    features = score_weight.shape[0]
    ratio = QUERY_HEADS // KV_HEAD_COUNT
    block = pl.BlockSpec((chunks, slot, width), lambda r, *_: (0, r, 0))
    attention, reward = pl.pallas_call(
        functools.partial(attend_kernel, features // (ratio * HEAD_SIZE), chunks),
        grid_spec=pltpu.PrefetchScalarGridSpec(
            num_scalar_prefetch=2,
            grid=(rollouts,),
            in_specs=[pl.BlockSpec((1, features), lambda r, *_: (0, 0)), block, block],
            out_specs=[
                pl.BlockSpec((slot, features), lambda r, *_: (r, 0)),
                pl.BlockSpec((1, 8, HEAD_SIZE), lambda r, *_: (r, 0, 0)),
            ],
        ),
        out_shape=[
            jax.ShapeDtypeStruct((rows, features), jnp.bfloat16),
            jax.ShapeDtypeStruct((rollouts, 8, HEAD_SIZE), jnp.float32),
        ],
    )(lengths, flag, score_weight.reshape(1, features), own, extra)
    return attention, reward[:, 0, 0]


def project_kernel(
    n, tp_count, tokens, weight, own_out, extra, gath, far, prod,
    tok_v, far_v, w_v, acc, pbuf, send, recv, loads, w_sem, misc,
):
    g = lax.axis_index("grp")
    t = lax.axis_index("tp")
    z, core = g // CORES, g % CORES
    rows, depth = tokens.shape
    chunks, _, width = gath.shape
    own_rows = weight.shape[0]
    half = own_rows * tp_count
    plane = half * CORES
    columns = width * chunks
    part = rows // tp_count
    far_cols = far.shape[1]
    steps = n - 2
    inner = (z >= 1) & (z <= n - 2)
    helper = (z == 1) | (z == n - 2)
    at_end = (z == 0) | (z == n - 1)
    first_far = jnp.where(z < n // 2, 2, 0)
    ids = {}

    def sem(key):
        return ids.setdefault(key, len(ids))

    def remote(key, src, dst, device):
        i = sem(key)
        return pltpu.make_async_remote_copy(
            src_ref=src, dst_ref=dst, send_sem=send.at[i], recv_sem=recv.at[i],
            device_id=device, device_id_type=pl.DeviceIdType.MESH,
        )

    sends = []

    def start(cond, key, src, dst, device):
        @pl.when(cond)
        def _():
            remote(key, src, dst, device).start()

        sends.append((cond, key, src, dst, device))

    def arrived(cond, key, dst):
        @pl.when(cond)
        def _():
            remote(key, dst, dst, (g, t)).wait_recv()

    always = z >= 0
    sibling = (g + 1 - 2 * core, t)

    def piece(q, who):
        return gath.at[q, pl.ds(pl.multiple_of(z * plane + core * half + who * own_rows, own_rows), own_rows)]

    def block(q, p, c):
        return gath.at[q, pl.ds(pl.multiple_of(p * plane + c * half, half), half)]

    def columns_of(who, q):
        return weight.at[:, pl.ds(pl.multiple_of(who * columns + q * width, width), width)]

    def scatter(q):
        pltpu.make_async_copy(columns_of(t, q), piece(q, t), loads.at[q]).start()
        for d in range(1, tp_count):
            start(always, ("a", q, d), columns_of(t ^ d, q), piece(q, t), (g, t ^ d))

    def gathered(q):
        pltpu.make_async_copy(columns_of(t, q), piece(q, t), loads.at[q]).wait()
        for d in range(1, tp_count):
            arrived(always, ("a", q, d), piece(q, t ^ d))

    def launch(q):
        mine = block(q, z, core)
        start(z >= 1, ("l", q, 1), mine, mine, (g - CORES, t))
        start(z <= n - 2, ("r", q, 1), mine, mine, (g + CORES, t))
        start(always, ("s", q), mine, mine, sibling)

    def has(side, s):
        reach = (z + s <= n - 1) if side == "l" else (z - s >= 0)
        return reach if s == 1 else reach & inner

    def forward(q, s):
        for side, sign in (("l", 1), ("r", -1)):
            here = jnp.clip(z + sign * s, 0, n - 1)
            got = block(q, here, core)
            arrived(has(side, s), (side, q, s), got)
            if s < steps:
                more = (z >= 2) if side == "l" else (z <= n - 3)
                start(has(side, s) & more, (side, q, s + 1), got, got, (g - sign * CORES, t))
            start(has(side, s), ("s" + side, q, s), got, got, sibling)

    def swapped(q):
        arrived(always, ("s", q), block(q, z, 1 - core))
        for s in range(1, steps + 1):
            for side, sign in (("l", 1), ("r", -1)):
                here = jnp.clip(z + sign * s, 0, n - 1)
                arrived(has(side, s), ("s" + side, q, s), block(q, here, 1 - core))

    tile = 256

    def gemm(q, lhs, low, high, origin):
        def load(p):
            return pltpu.make_async_copy(
                gath.at[q, pl.ds(pl.multiple_of(p * plane, plane), plane)], w_v.at[p % 2], w_sem.at[p % 2]
            )

        load(low).start()
        acc[...] = jnp.zeros_like(acc)

        def step(p, carry):
            @pl.when(p + 1 < high)
            def _():
                load(p + 1).start()

            load(p).wait()
            cols = pl.ds(pl.multiple_of((p - origin) * plane, plane), plane)

            def rows_step(m, carry):
                at = pl.ds(pl.multiple_of(m * tile, tile), tile)
                acc[at, :] += jnp.dot(lhs[at, cols], w_v[p % 2], preferred_element_type=jnp.float32)
                return carry

            return lax.fori_loop(0, rows // tile, rows_step, carry)

        lax.fori_loop(low, high, step, 0)

    def compute(q):
        low = jnp.where(z == n - 1, n - 2, 0)
        high = jnp.where(z == 0, 2, n)
        gemm(q, tok_v, low, high, 0)
        out = pltpu.make_async_copy(acc, own_out.at[q], misc.at[1])
        out.start()
        out.wait()

    def assist(q):
        @pl.when(helper)
        def _():
            gemm(q, far_v, first_far, first_far + steps, first_far)
            pbuf[...] = acc[...].astype(pbuf.dtype)
            out = pltpu.make_async_copy(pbuf, prod.at[q], misc.at[2])
            out.start()
            out.wait()

        start(helper, ("p", q), prod.at[q], extra.at[q], (jnp.where(z == 1, g - CORES, g + CORES), t))

    def token_rows(who):
        return far.at[pl.ds(pl.multiple_of(who * part, part), part)]

    load_tokens = pltpu.make_async_copy(tokens, tok_v, misc.at[0])
    far_source = tokens.at[
        pl.ds(pl.multiple_of(t * part, part), part),
        pl.ds(pl.multiple_of(first_far * plane, plane), far_cols),
    ]
    start(at_end, ("t",), far_source, token_rows(t), (jnp.where(z == 0, g + CORES, g - CORES), t))
    for q in range(chunks):
        scatter(q)
    load_tokens.start()
    for q in range(chunks):
        gathered(q)
        launch(q)
    arrived(helper, ("t",), token_rows(t))
    for d in range(1, tp_count):
        start(helper, ("g", d), token_rows(t), token_rows(t), (g, t ^ d))
    load_tokens.wait()
    for q in range(chunks - 1):
        forward(q, 1)
    for q in range(chunks):
        for s in range(2, steps + 1):
            forward(q, s)
        swapped(q)
        if q == 0:
            for d in range(1, tp_count):
                arrived(helper, ("g", d), token_rows(t ^ d))

            @pl.when(helper)
            def _():
                fill = pltpu.make_async_copy(far, far_v, misc.at[0])
                fill.start()
                fill.wait()

        assist(q)
        if q == 0:
            forward(chunks - 1, 1)
        compute(q)
    for q in range(chunks):
        arrived(at_end, ("p", q), extra.at[q])
    for cond, key, src, dst, device in sends:
        @pl.when(cond)
        def _():
            remote(key, src, dst, device).wait_send()


def project(tokens, weight, n, tp_count):
    rows, depth = tokens.shape
    own_rows = weight.shape[0]
    width = weight.shape[1] // tp_count // CHUNKS
    plane = own_rows * tp_count * CORES
    far = plane * (n - 2)
    flows = CHUNKS * (tp_count + 1 + 4 * (n - 2)) + tp_count
    anywhere = pl.BlockSpec(memory_space=pl.ANY)
    own, extra, *_ = pl.pallas_call(
        functools.partial(project_kernel, n, tp_count),
        in_specs=[anywhere] * 2,
        out_specs=[anywhere] * 5,
        out_shape=[
            jax.ShapeDtypeStruct((CHUNKS, rows, width), jnp.float32),
            jax.ShapeDtypeStruct((CHUNKS, rows, width), jnp.bfloat16),
            jax.ShapeDtypeStruct((CHUNKS, depth, width), jnp.bfloat16),
            jax.ShapeDtypeStruct((rows, far), jnp.bfloat16),
            jax.ShapeDtypeStruct((CHUNKS, rows, width), jnp.bfloat16),
        ],
        scratch_shapes=[
            pltpu.VMEM((rows, depth), jnp.bfloat16),
            pltpu.VMEM((rows, far), jnp.bfloat16),
            pltpu.VMEM((2, plane, width), jnp.bfloat16),
            pltpu.VMEM((rows, width), jnp.float32),
            pltpu.VMEM((rows, width), jnp.bfloat16),
            pltpu.SemaphoreType.DMA((flows,)),
            pltpu.SemaphoreType.DMA((flows,)),
            pltpu.SemaphoreType.DMA((CHUNKS,)),
            pltpu.SemaphoreType.DMA((2,)),
            pltpu.SemaphoreType.DMA((3,)),
        ],
        compiler_params=pltpu.CompilerParams(has_side_effects=True, vmem_limit_bytes=60 * 1024 * 1024),
    )(tokens, weight)
    return own, extra


def share_kernel(grp_count, tp_count, mine, out, held, send, recv, local):
    g = lax.axis_index("grp")
    t = lax.axis_index("tp")

    def copy(i, src, dst, device):
        return pltpu.make_async_remote_copy(
            src_ref=src, dst_ref=dst, send_sem=send.at[i], recv_sem=recv.at[i],
            device_id=device, device_id_type=pl.DeviceIdType.MESH,
        )

    own = pltpu.make_async_copy(mine, held.at[g, t], local)
    own.start()
    first = [copy(d - 1, mine, held.at[g, t], (g, t ^ d)) for d in range(1, tp_count)]
    for c in first:
        c.start()
    own.wait()
    for d in range(1, tp_count):
        copy(d - 1, mine, held.at[g, t ^ d], (g, t)).wait_recv()
    second = [
        copy(tp_count - 1 + d - 1, held.at[g], held.at[g], ((g + d) % grp_count, t))
        for d in range(1, grp_count)
    ]
    for c in second:
        c.start()
    for d in range(1, grp_count):
        source = held.at[(g + grp_count - d) % grp_count]
        copy(tp_count - 1 + d - 1, source, source, (g, t)).wait_recv()
    for c in first + second:
        c.wait_send()
    out[...] = held[...]


def share(mine, grp_count, tp_count):
    shape = (grp_count, tp_count) + mine.shape
    flows = grp_count + tp_count - 2
    return pl.pallas_call(
        functools.partial(share_kernel, grp_count, tp_count),
        in_specs=[pl.BlockSpec(memory_space=pl.ANY)],
        out_specs=pl.BlockSpec(memory_space=pltpu.VMEM),
        out_shape=jax.ShapeDtypeStruct(shape, mine.dtype),
        scratch_shapes=[
            pltpu.VMEM(shape, mine.dtype),
            pltpu.SemaphoreType.DMA((flows,)),
            pltpu.SemaphoreType.DMA((flows,)),
            pltpu.SemaphoreType.DMA,
        ],
        compiler_params=pltpu.CompilerParams(has_side_effects=True),
    )(mine)


def shards(tokens, joined_weight, rollout_lengths, prompt_of, score_weight):
    grp_count = lax.axis_size("grp")
    tp_count = lax.axis_size("tp")
    n = grp_count // CORES
    g = lax.axis_index("grp")
    z = g // CORES
    own, extra = project(tokens, joined_weight, n, tp_count)
    flag = ((z == 0) | (z == n - 1)).astype(jnp.int32).reshape(1)
    attention, reward = attend(own, extra, rollout_lengths, flag, score_weight)
    reward = reward / rollout_lengths.astype(jnp.float32)
    sent = jnp.stack([reward, prompt_of[:, 0].astype(jnp.float32)])
    count = reward.shape[0]
    sent = jnp.pad(sent, ((0, -2 % 8), (0, -count % 128)))
    gathered = share(sent, grp_count, tp_count)[:, :, :2, :count]
    everyone = jnp.sum(gathered[:, :, 0], axis=1).reshape(-1)
    prompts = gathered[:, 0, 1].reshape(-1, 1).astype(jnp.int32)
    labels = jnp.arange(grp_count)[None, :]
    onehot = (prompts == labels).astype(jnp.float32)
    counts = jnp.sum(onehot, axis=0)
    totals = jnp.sum(onehot * everyone[:, None], axis=0)
    squares = jnp.sum(onehot * (everyone * everyone)[:, None], axis=0)
    divisor = jnp.maximum(counts, 1.0)
    average = totals / divisor
    spread = squares / divisor - average * average
    mine = (prompt_of == labels).astype(jnp.float32)
    own_mean = jnp.sum(mine * average[None, :], axis=1)
    own_var = jnp.sum(mine * spread[None, :], axis=1)
    rewards = lax.dynamic_slice(everyone, (g * reward.shape[0],), reward.shape)
    advantages = (rewards - own_mean) / jnp.sqrt(own_var + 0.25)
    return (attention, advantages)


def solution(mesh):
    return jax.shard_map(
        shards,
        mesh=mesh,
        in_specs=(P("grp", None), P(("grp", "tp"), None), P("grp"), P("grp", None), P("tp")),
        out_specs=(P("grp", "tp"), P("grp")),
        check_vma=False,
    )
```
